32 devices in a mesh: grp: 2 (over core), row: 4 (over z), col: 4 (over y, x).
Axes of the slice: x: 2, y: 2, z: 4, core: 2. Of those that a mesh axis runs over, the one named last changes fastest.
Arguments:
- ainv_anc: bfloat16 [6144, 6144], P(('grp', 'row'), 'col'), may hold values from -12 to 12
- l_upper: bfloat16 [6144, 1024], P(('grp', 'row'), 'col'), may hold values from -0.078125 to 0.078125
- mask_upper: int32 [4, 24], replicated, may hold values from 0 to 1, as said below
- dinv_upper: float32 [256, 1024], P(None, 'col'), may hold values from -6 to 6
- l_lower: bfloat16 [6144, 1024], P(('grp', 'row'), 'col'), may hold values from -0.078125 to 0.078125
- mask_lower: int32 [4, 24], replicated, may hold values from 0 to 1, as said below
- parent: int32 [4], replicated, may hold values from 0 to 3
- lp_lower: bfloat16 [256, 1024], P(None, 'col'), may hold values from -0.375 to 0.375
- dinv_lower: float32 [256, 1024], P(None, 'col'), may hold values from -6 to 6
Outputs:
- x_upper: bfloat16 [6144, 1024], P(('grp', 'row'), 'col')
- diag_upper: bfloat16 [256, 1024], P(None, 'col')
- y_lower: bfloat16 [6144, 1024], P(('grp', 'row'), 'col')
- y_parent: bfloat16 [256, 1024], P(None, 'col')
- diag_lower: bfloat16 [256, 1024], P(None, 'col')
The draws below stay inside these ranges and needn't reach their ends.
Inputs may be any that keep to these rules, and one draw needn't show every extreme that they name: mask_upper[u, a] is 1 where ancestor block a lies in the structure of upper supernode u. mask_lower[l, a] is 1 where ancestor block a lies in the structure of lower supernode l. parent[l] is the upper supernode whose columns hold lower supernode l's parent block.
All inputs are finite; a program needn't handle non-finite values.
Results may differ from the reference program's by a relative error of at most 0.0095.
Values may be sent and summed in bfloat16 or wider, within the bound.
A program may use at most 128 MiB of HBM per device.

```python
import jax
import jax.numpy as jnp
from jax import lax

B = 256
ANC = 6144
ANCB = 24
SN = 4


def draw_ainv_anc(key, part):
    entry_key, diag_key = jax.random.split(key, 2)
    entries = jnp.clip(jax.random.normal(entry_key, (ANC, ANC), jnp.float32), -7.0, 7.0)
    diagonal = jnp.exp(jax.random.uniform(diag_key, (ANC,), jnp.float32, 0.0, 1.386))
    places = jnp.arange(ANC)
    return entries.at[places, places].add(diagonal).astype(jnp.bfloat16)


def pattern_draw(key):
    chance = jax.random.randint(key, (SN, ANCB), 0, 1000)
    threshold = 250 + 650 * jnp.arange(ANCB, dtype=jnp.int32) // max(ANCB - 1, 1)
    return (chance < threshold[None, :]).astype(jnp.int32)


def draw_mask_upper(key, part):
    return pattern_draw(jax.random.fold_in(key, 17))


def draw_mask_lower(key, part):
    return pattern_draw(jax.random.fold_in(key, 29))


def plant(drawn, own_key, smallest, high):
    dims = drawn.shape
    place = [jax.random.randint(jax.random.fold_in(own_key, axis), (), 0, dims[axis]) for axis in range(len(dims))]
    drawn = drawn.at[tuple(place)].set(smallest)
    longest = dims.index(max(dims))
    place[longest] = (place[longest] + 1) % dims[longest]
    return drawn.at[tuple(place)].set(high)


def levels(stream_key, shape, cuts, smallest, high):
    def one(position, shards_of):
        heights = jax.random.uniform(jax.random.fold_in(jax.random.fold_in(stream_key, 6), position), (shards_of,), jnp.float32, smallest / len(cuts), high / len(cuts))
        return jnp.repeat(jnp.exp(heights), shape[position] // shards_of).reshape((-1,) + (1,) * (len(shape) - position - 1))

    gain = one(*cuts[0])
    for cut in cuts[1:]:
        gain = gain * one(*cut)
    return gain


def noise(rng, extent, width, bound, cuts=(), kind=jnp.bfloat16):
    values = jax.random.normal(rng, extent, jnp.float32) * width
    if len(cuts) > 0:
        values = levels(rng, extent, cuts, -0.22, 0.18) * values
    return jnp.clip(values, min=-bound, max=bound).astype(kind)


def setup_inputs(seed: int = 0) -> dict:
    keys = jax.random.split(jax.random.key(seed), 10)
    return {
        "ainv_anc": draw_ainv_anc(jax.random.fold_in(keys[9], 71), 0),
        "l_upper": noise(keys[1], (ANC, SN * B), ANC ** -0.5, 0.078125, ((0, 8), (1, 4))),
        "mask_upper": draw_mask_upper(jax.random.fold_in(keys[9], 71), 0),
        "dinv_upper": noise(keys[3], (B, SN * B), 1.0, 6.0, ((1, 4),), jnp.float32),
        "l_lower": noise(keys[4], (ANC, SN * B), ANC ** -0.5, 0.078125, ((0, 8), (1, 4))),
        "mask_lower": draw_mask_lower(jax.random.fold_in(keys[9], 71), 0),
        "parent": plant(jax.random.randint(keys[6], (SN,), 0, SN), jax.random.fold_in(keys[6], 1), 0, SN - 1).astype(jnp.int32),
        "lp_lower": noise(keys[7], (B, SN * B), B ** -0.5, 0.375, ((1, 4),)),
        "dinv_lower": noise(keys[8], (B, SN * B), 1.0, 6.0, ((1, 4),), jnp.float32),
    }


def masked_panel(factor, pattern):
    height, breadth = factor.shape
    shaped = factor.reshape(height // B, B, breadth // B, B)
    keeping = (jnp.transpose(pattern) > 0)[:, None, :, None]
    return jnp.where(keeping, shaped, jnp.zeros((), factor.dtype)).reshape(height, breadth)


def reference(ainv_anc, l_upper, mask_upper, dinv_upper, l_lower, mask_lower, parent, lp_lower, dinv_lower):
    precise = lax.Precision.HIGHEST
    ancestor = ainv_anc.astype(jnp.float32)
    upper_masked = masked_panel(l_upper, mask_upper)
    x_upper = (-jnp.dot(ancestor, upper_masked.astype(jnp.float32), precision=precise)).astype(jnp.bfloat16)
    upper_cube = upper_masked.astype(jnp.float32).reshape(ANC, SN, B)
    x_cube = x_upper.astype(jnp.float32).reshape(ANC, SN, B)
    upper_terms = jnp.einsum("aub,auc->buc", upper_cube, x_cube, precision=precise).reshape(B, SN * B)
    diag_upper = (dinv_upper - upper_terms).astype(jnp.bfloat16)
    lower_masked = masked_panel(l_lower, mask_lower)
    lower_cube = lower_masked.astype(jnp.float32).reshape(ANC, SN, B)
    chosen = jnp.take(x_cube, parent, axis=1)
    link_cube = lp_lower.astype(jnp.float32).reshape(B, SN, B)
    coupling = jnp.einsum("alb,blc->alc", chosen, link_cube, precision=precise).reshape(ANC, SN * B)
    lower_sum = jnp.dot(ancestor, lower_masked.astype(jnp.float32), precision=precise)
    y_lower = (-(lower_sum + coupling)).astype(jnp.bfloat16)
    y_cube = y_lower.astype(jnp.float32).reshape(ANC, SN, B)
    crossed = jnp.einsum("alb,alc->blc", chosen, lower_cube, precision=precise)
    own_terms = jnp.einsum("alb,alc->blc", lower_cube, y_cube, precision=precise)
    parent_diag = jnp.take(diag_upper.astype(jnp.float32).reshape(B, SN, B), parent, axis=1)
    parent_terms = jnp.einsum("blc,cld->bld", parent_diag, link_cube, precision=precise)
    y_parent = (-(crossed + parent_terms)).astype(jnp.bfloat16)
    parent_cube = y_parent.astype(jnp.float32)
    back_terms = jnp.einsum("clb,cld->bld", link_cube, parent_cube, precision=precise)
    diag_lower = (dinv_lower.reshape(B, SN, B) - own_terms - back_terms).astype(jnp.bfloat16)
    return x_upper, diag_upper, y_lower, y_parent.reshape(B, SN * B), diag_lower.reshape(B, SN * B)
```

```python
import functools

import jax
import jax.numpy as jnp
from jax import lax
from jax.experimental import pallas as pl
from jax.experimental.pallas import tpu as pltpu
from jax.sharding import PartitionSpec as P

B = 256
MESH = pl.DeviceIdType.MESH
BF = jnp.bfloat16
F32 = jnp.float32


def tdot(a, b):
    return lax.dot_general(a, b, (((0,), (0,)), ((), ())), preferred_element_type=F32)


def kernel(
    G, R, C,
    a_ref, lu_ref, mu_ref, du_ref, ll_ref, ml_ref, par_ref, lp_ref, dl_ref,
    x_ref, diagu_ref, y_ref, yp_ref, diagl_ref,
    zbuf, col, part, rsb, acc, xall, rhs, lum, llm, part3, red, dufull, dpar, ypfull, ownfull,
    own_ss, z_ss, z_rs, p_ss, c_rs, r_ss, rs_ss, rs_rs, x_ss, x_rs, red_ss, red_rs,
    d_ss, d_rs, dp_ss, dp_rs, y_ss, y_rs, o_ss, o_rs,
):
    g, z, c = lax.axis_index("grp"), lax.axis_index("row"), lax.axis_index("col")
    n = G * R
    q = n // C
    r = g * R + z
    h = lu_ref.shape[0]
    hb = h // B
    S = B // n
    panels = (lu_ref, ll_ref)
    masks = (mu_ref, ml_ref)
    primary = (c * q) // R == g

    def rdev(i):
        return (lax.div(i, R), lax.rem(i, R), c)

    def copy(src, dst, ss, rs, dev):
        return pltpu.make_async_remote_copy(
            src_ref=src, dst_ref=dst, send_sem=ss, recv_sem=rs, device_id=dev, device_id_type=MESH
        )

    barrier = pltpu.get_barrier_semaphore()
    for o in range(1, n):
        pl.semaphore_signal(barrier, inc=1, device_id=rdev(lax.rem(r + o, n)), device_id_type=MESH)
    for o in range(1, C):
        pl.semaphore_signal(
            barrier, inc=1, device_id=(g, z, lax.rem(c + o, C)), device_id_type=MESH
        )
    pl.semaphore_wait(barrier, n - 1 + C - 1)

    def own_copy(p, side):
        to = z + 1 if side == 0 else z - 1
        return copy(panels[p], zbuf.at[p, z], own_ss.at[p, side], z_rs.at[p, z], (g, to, c))

    def fwd_copy(p, z0, side):
        to = z + 1 if side == 0 else z - 1
        return copy(zbuf.at[p, z0], zbuf.at[p, z0], z_ss.at[p, z0], z_rs.at[p, z0], (g, to, c))

    def plane_copy(p, z0, src):
        r0 = g * R + z0
        return copy(
            src, col.at[p, lax.rem(r0, q), c], p_ss.at[p, z0], c_rs.at[p, lax.rem(r0, q), c],
            (g, z, lax.div(r0, q)),
        )

    def relay_copy(p, j, u):
        return copy(
            col.at[p, j, u], col.at[p, j, u], r_ss.at[p, j, u], c_rs.at[p, j, u], (1 - g, z, c)
        )

    def to_plane(p, z0, src):
        r0 = g * R + z0
        d = lax.div(r0, q)

        @pl.when(d == c)
        def _():
            j = lax.rem(r0, q)
            pltpu.make_async_copy(src, col.at[p, j, c], c_rs.at[p, j, c]).start()

        @pl.when(d != c)
        def _():
            plane_copy(p, z0, src).start()

    def start_own(p):
        @pl.when(z < R - 1)
        def _():
            own_copy(p, 0).start()

        @pl.when(z > 0)
        def _():
            own_copy(p, 1).start()

        to_plane(p, z, panels[p])

    def relay(p, z0):
        r0 = g * R + z0

        @pl.when(lax.div(r0, q) == c)
        def _():
            j = lax.rem(r0, q)
            for o in range(C):
                u = lax.rem(c + o, C)
                relay_copy(p, j, u).wait_recv()
                relay_copy(p, j, u).start()

    def relay_step(p, s):
        if s == 0:
            relay(p, z)
            return

        @pl.when(z - s >= 0)
        def _():
            relay(p, z - s)

        @pl.when(z + s < R)
        def _():
            relay(p, z + s)

    def row_step(p, s):
        zl, zr = z - s, z + s

        @pl.when(zl >= 0)
        def _():
            fwd_copy(p, zl, 0).wait_recv()

            @pl.when(z < R - 1)
            def _():
                fwd_copy(p, zl, 0).start()

            to_plane(p, zl, zbuf.at[p, zl])

        @pl.when(zr < R)
        def _():
            fwd_copy(p, zr, 1).wait_recv()

            @pl.when(z > 0)
            def _():
                fwd_copy(p, zr, 1).start()

            to_plane(p, zr, zbuf.at[p, zr])

        relay_step(p, s - 1)

    def part_copy(p, o):
        u = lax.rem(c + o, C)
        return copy(part.at[p, o - 1], rsb.at[p, c], rs_ss.at[p, o], rs_rs.at[p, c], (g, z, u))

    def products(p):
        relay_step(p, R - 1)

        @pl.when(jnp.logical_not(primary))
        def _():
            for j in range(q):
                for u in range(C):
                    relay_copy(p, j, u).wait_recv()

        for o in list(range(1, C)) + [0]:
            u = lax.rem(c + o, C)

            @pl.loop(0, q * hb)
            def _(k):
                j, t = lax.div(k, hb), lax.rem(k, hb)
                keep = masks[p][u, c * q * hb + k] > 0
                rows = pl.ds(pl.multiple_of(t * B, B), B)
                blk = col[p, j, u, rows, :]
                rhs[pl.ds(pl.multiple_of(k * B, B), B), :] = jnp.where(
                    keep, blk, jnp.zeros_like(blk)
                )

            @pl.loop(0, hb)
            def _(t):
                rows = pl.ds(pl.multiple_of(t * B, B), B)
                v = jnp.dot(a_ref[rows, :], rhs[...], preferred_element_type=F32)
                if o == 0:
                    acc[p, rows, :] = v
                else:
                    part[p, o - 1, rows, :] = v.astype(BF)

            if o != 0:
                part_copy(p, o).start()

    def wait_parts(p):
        for o in range(1, C):
            s = lax.rem(c + o, C)
            copy(
                rsb.at[p, s], rsb.at[p, s], rs_ss.at[p, o], rs_rs.at[p, s], (g, z, s)
            ).wait_recv()

    def total(p, rows):
        v = acc[p, rows, :]
        for o in range(1, C):
            v = v + rsb[p, lax.rem(c + o, C), rows, :].astype(F32)
        return v

    def red_copy(k, o):
        i = lax.rem(r + o, n)
        return copy(
            part3.at[k, pl.ds(pl.multiple_of(i * S, S), S), :], red.at[k, r],
            red_ss.at[k, o], red_rs.at[k, r], rdev(i),
        )

    def send_sum(k):
        red[k, r] = part3[k, pl.ds(pl.multiple_of(r * S, S), S), :]
        for o in range(1, n):
            red_copy(k, o).start()

    def take_sum(k):
        for o in range(1, n):
            s = lax.rem(r + o, n)
            copy(
                red.at[k, s], red.at[k, s], red_ss.at[k, o], red_rs.at[k, s], rdev(s)
            ).wait_recv()
        v = red[k, 0]
        for i in range(1, n):
            v = v + red[k, i]
        return v

    mine = pl.ds(pl.multiple_of(r * S, S), S)

    def spread_copy(buf, ss, rs, o):
        return copy(buf.at[mine, :], buf.at[mine, :], ss.at[o], rs.at[r], rdev(lax.rem(r + o, n)))

    def spread(buf, ss, rs):
        for o in range(1, n):
            spread_copy(buf, ss, rs, o).start()

    def gathered(buf, ss, rs):
        for o in range(1, n):
            s = lax.rem(r + o, n)
            at = buf.at[pl.ds(pl.multiple_of(s * S, S), S), :]
            copy(at, at, ss.at[o], rs.at[s], rdev(s)).wait_recv()

    def x_copy(o):
        return copy(xall.at[c], xall.at[c], x_ss.at[o], x_rs.at[c], (g, z, lax.rem(c + o, C)))

    def dp_copy(o):
        return copy(dpar.at[c], dpar.at[c], dp_ss.at[o], dp_rs.at[c], (g, z, lax.rem(c + o, C)))

    start_own(0)

    @pl.loop(0, hb)
    def _(t):
        rows = pl.ds(pl.multiple_of(t * B, B), B)
        ub, lb = lu_ref[rows, :], ll_ref[rows, :]
        lum[rows, :] = jnp.where(mu_ref[c, r * hb + t] > 0, ub, jnp.zeros_like(ub))
        llm[rows, :] = jnp.where(ml_ref[c, r * hb + t] > 0, lb, jnp.zeros_like(lb))

    for s in range(1, R):
        row_step(0, s)
    start_own(1)
    row_step(1, 1)
    products(0)
    for s in range(2, R):
        row_step(1, s)

    wait_parts(0)

    @pl.loop(0, hb)
    def _(t):
        rows = pl.ds(pl.multiple_of(t * B, B), B)
        v = (-total(0, rows)).astype(BF)
        xall[c, rows, :] = v
        x_ref[rows, :] = v

    for o in range(1, C):
        x_copy(o).start()

    products(1)

    part3[0] = tdot(lum[...], x_ref[...])
    send_sum(0)

    for o in range(1, C):
        s = lax.rem(c + o, C)
        copy(xall.at[s], xall.at[s], x_ss.at[o], x_rs.at[s], (g, z, s)).wait_recv()
    here = par_ref[c]
    part3[1] = tdot(xall[here], llm[...])
    send_sum(1)

    dslice = (du_ref[mine, :] - take_sum(0)).astype(BF)
    dufull[mine, :] = dslice
    dpar[c] = dslice
    for o in range(1, C):
        dp_copy(o).start()
    spread(dufull, d_ss, d_rs)

    @pl.loop(0, hb)
    def _(t):
        rows = pl.ds(pl.multiple_of(t * B, B), B)
        acc[1, rows, :] += jnp.dot(xall[here, rows, :], lp_ref[...], preferred_element_type=F32)

    for o in range(1, C):
        s = lax.rem(c + o, C)
        copy(dpar.at[s], dpar.at[s], dp_ss.at[o], dp_rs.at[s], (g, z, s)).wait_recv()
    terms = jnp.dot(dpar[here], lp_ref[...], preferred_element_type=F32)
    ypfull[mine, :] = (-(take_sum(1) + terms)).astype(BF)
    spread(ypfull, y_ss, y_rs)

    wait_parts(1)

    @pl.loop(0, hb)
    def _(t):
        rows = pl.ds(pl.multiple_of(t * B, B), B)
        y_ref[rows, :] = (-total(1, rows)).astype(BF)

    part3[2] = tdot(llm[...], y_ref[...])
    send_sum(2)
    gathered(ypfull, y_ss, y_rs)
    back = tdot(lp_ref[...], ypfull[...])
    yp_ref[...] = ypfull[...]
    gathered(dufull, d_ss, d_rs)
    diagu_ref[...] = dufull[...]
    ownfull[mine, :] = take_sum(2)
    spread(ownfull, o_ss, o_rs)
    gathered(ownfull, o_ss, o_rs)
    diagl_ref[...] = (dl_ref[...] - ownfull[...] - back).astype(BF)

    for p in range(2):
        @pl.when(z < R - 1)
        def _():
            own_copy(p, 0).wait_send()

        @pl.when(z > 0)
        def _():
            own_copy(p, 1).wait_send()

        for z0 in range(R):
            @pl.when(jnp.logical_and(z0 < z, z < R - 1))
            def _():
                fwd_copy(p, z0, 0).wait_send()

            @pl.when(jnp.logical_and(z0 > z, z > 0))
            def _():
                fwd_copy(p, z0, 1).wait_send()

            @pl.when(lax.div(g * R + z0, q) != c)
            def _():
                plane_copy(p, z0, zbuf.at[p, z0]).wait_send()

        @pl.when(primary)
        def _():
            for j in range(q):
                for u in range(C):
                    relay_copy(p, j, u).wait_send()

        for o in range(1, C):
            part_copy(p, o).wait_send()
    for o in range(1, C):
        x_copy(o).wait_send()
        dp_copy(o).wait_send()
    for o in range(1, n):
        for k in range(3):
            red_copy(k, o).wait_send()
        spread_copy(dufull, d_ss, d_rs, o).wait_send()
        spread_copy(ypfull, y_ss, y_rs, o).wait_send()
        spread_copy(ownfull, o_ss, o_rs, o).wait_send()


def on_device(G, R, C, a, lu, mu, du, ll, ml, par, lp, dl):
    h = lu.shape[0]
    n = G * R
    q = n // C
    S = B // n
    vm = pl.BlockSpec(memory_space=pltpu.VMEM)
    sm = pl.BlockSpec(memory_space=pltpu.SMEM)
    dma = pltpu.SemaphoreType.DMA
    small = jax.ShapeDtypeStruct((B, B), BF)
    tall = jax.ShapeDtypeStruct((h, B), BF)
    return pl.pallas_call(
        functools.partial(kernel, G, R, C),
        out_shape=(tall, small, tall, small, small),
        in_specs=[vm, vm, sm, vm, vm, sm, sm, vm, vm],
        out_specs=(vm,) * 5,
        scratch_shapes=[
            pltpu.VMEM((2, R, h, B), BF),
            pltpu.VMEM((2, q, C, h, B), BF),
            pltpu.VMEM((2, C - 1, h, B), BF),
            pltpu.VMEM((2, C, h, B), BF),
            pltpu.VMEM((2, h, B), F32),
            pltpu.VMEM((C, h, B), BF),
            pltpu.VMEM((q * h, B), BF),
            pltpu.VMEM((h, B), BF),
            pltpu.VMEM((h, B), BF),
            pltpu.VMEM((3, B, B), F32),
            pltpu.VMEM((3, n, S, B), F32),
            pltpu.VMEM((B, B), BF),
            pltpu.VMEM((C, S, B), BF),
            pltpu.VMEM((B, B), BF),
            pltpu.VMEM((B, B), F32),
            dma((2, 2)), dma((2, R)), dma((2, R)), dma((2, R)), dma((2, q, C)), dma((2, q, C)),
            dma((2, C)), dma((2, C)), dma((C,)), dma((C,)), dma((3, n)), dma((3, n)),
            dma((n,)), dma((n,)), dma((C,)), dma((C,)), dma((n,)), dma((n,)), dma((n,)), dma((n,)),
        ],
        compiler_params=pltpu.CompilerParams(
            collective_id=0, has_side_effects=True, vmem_limit_bytes=60 * 1024 * 1024
        ),
    )(a, lu, mu, du, ll, ml, par, lp, dl)


def solution(mesh):
    tall, wide = P(("grp", "row"), "col"), P(None, "col")
    return jax.shard_map(
        functools.partial(
            on_device, mesh.shape["grp"], mesh.shape["row"], mesh.shape["col"]
        ),
        mesh=mesh,
        in_specs=(tall, tall, P(), wide, tall, P(), P(), wide, wide),
        out_specs=(tall, wide, tall, wide, wide),
        check_vma=False,
    )
```

```python
import functools

import jax
import jax.numpy as jnp
from jax import lax
from jax.experimental import pallas as pl
from jax.experimental.pallas import tpu as pltpu
from jax.sharding import PartitionSpec as P

B = 256
MESH = pl.DeviceIdType.MESH
BF = jnp.bfloat16
F32 = jnp.float32


def tdot(a, b):
    return lax.dot_general(a, b, (((0,), (0,)), ((), ())), preferred_element_type=F32)


def kernel(
    G, R, C,
    a_ref, lu_ref, mu_ref, du_ref, ll_ref, ml_ref, par_ref, lp_ref, dl_ref,
    x_ref, diagu_ref, y_ref, yp_ref, diagl_ref,
    zbuf, col, part, near, sent, last, acc, xall, rhs, lum, llm, part3, red, dufull, dpar,
    ypfull, ownfull,
    pre_ss, z_ss, z_rs, p_ss, c_rs, r_ss, n_ss, n_rs, l_ss, l_rs, x_ss, x_rs, xy_ss,
    red_ss, red_rs, d_ss, d_rs, dp_ss, dp_rs, y_ss, y_rs, o_ss, o_rs,
):
    g, z, c = lax.axis_index("grp"), lax.axis_index("row"), lax.axis_index("col")
    n = G * R
    q = n // C
    CX = C // G
    y, x = lax.div(c, CX), lax.rem(c, CX)
    r = g * R + z
    h = lu_ref.shape[0]
    hb = h // B
    S = B // n
    panels = (lu_ref, ll_ref)
    masks = (mu_ref, ml_ref)
    primary = y == g

    def rdev(i):
        return (lax.div(i, R), lax.rem(i, R), c)

    def copy(src, dst, ss, rs, dev):
        return pltpu.make_async_remote_copy(
            src_ref=src, dst_ref=dst, send_sem=ss, recv_sem=rs, device_id=dev, device_id_type=MESH
        )

    barrier = pltpu.get_barrier_semaphore()
    for o in range(1, n):
        pl.semaphore_signal(barrier, inc=1, device_id=rdev(lax.rem(r + o, n)), device_id_type=MESH)
    for o in range(1, C):
        pl.semaphore_signal(
            barrier, inc=1, device_id=(g, z, lax.rem(c + o, C)), device_id_type=MESH
        )
    pl.semaphore_wait(barrier, n - 1 + C - 1)

    def pre_copy(p):
        return copy(
            panels[p], zbuf.at[p, z, y], pre_ss.at[p], z_rs.at[p, z, y], (g, z, g * CX + x)
        )

    def row_copy(p, z0, yy, side, src=None):
        to = z + 1 if side == 0 else z - 1
        at = zbuf.at[p, z0, yy]
        return copy(
            at if src is None else src, at, z_ss.at[p, z0, yy, side], z_rs.at[p, z0, yy], (g, to, c)
        )

    def plane_copy(p, z0, yy, src):
        r0 = g * R + z0
        u = yy * CX + x
        return copy(
            src, col.at[p, lax.rem(r0, q), u], p_ss.at[p, z0, yy], c_rs.at[p, lax.rem(r0, q), u],
            (g, z, lax.div(r0, q)),
        )

    def relay_copy(p, j, u):
        return copy(
            col.at[p, j, u], col.at[p, j, u], r_ss.at[p, j, u], c_rs.at[p, j, u], (1 - g, z, c)
        )

    def to_plane(p, z0, yy, src):
        r0 = g * R + z0
        d = lax.div(r0, q)

        @pl.when(d == c)
        def _():
            j = lax.rem(r0, q)
            u = yy * CX + x
            pltpu.make_async_copy(src, col.at[p, j, u], c_rs.at[p, j, u]).start()

        @pl.when(d != c)
        def _():
            plane_copy(p, z0, yy, src).start()

    def pass_on(p, z0, yy, sides, src=None):
        if 0 in sides:
            @pl.when(z < R - 1)
            def _():
                row_copy(p, z0, yy, 0, src).start()

        if 1 in sides:
            @pl.when(z > 0)
            def _():
                row_copy(p, z0, yy, 1, src).start()

        to_plane(p, z0, yy, zbuf.at[p, z0, yy] if src is None else src)

    def start_own(p):
        pass_on(p, z, g, (0, 1), panels[p])
        row_copy(p, z, 1 - g, 0).wait_recv()
        pass_on(p, z, 1 - g, (0, 1))

    def relay(p, z0):
        r0 = g * R + z0

        @pl.when(lax.div(r0, q) == c)
        def _():
            j = lax.rem(r0, q)
            for o in range(CX):
                for yy in range(G):
                    u = yy * CX + lax.rem(x + o, CX)
                    relay_copy(p, j, u).wait_recv()
                    relay_copy(p, j, u).start()

    def relay_step(p, s):
        if s == 0:
            relay(p, z)
            return

        @pl.when(z - s >= 0)
        def _():
            relay(p, z - s)

        @pl.when(z + s < R)
        def _():
            relay(p, z + s)

    def row_step(p, s):
        zl, zr = z - s, z + s

        @pl.when(zl >= 0)
        def _():
            for i in range(G):
                yy = lax.rem(g + i, G)
                row_copy(p, zl, yy, 0).wait_recv()
                pass_on(p, zl, yy, (0,))

        @pl.when(zr < R)
        def _():
            for i in range(G):
                yy = lax.rem(g + i, G)
                row_copy(p, zr, yy, 1).wait_recv()
                pass_on(p, zr, yy, (1,))

        relay_step(p, s - 1)

    def near_copy(p, ux):
        return copy(
            part.at[p, ux], near.at[p, ux], n_ss.at[p, ux], n_rs.at[p, ux], (g, z, (1 - y) * CX + x)
        )

    def last_copy(p, ux):
        return copy(
            sent.at[p, ux], last.at[p, x], l_ss.at[p, ux], l_rs.at[p, x], (g, z, y * CX + ux)
        )

    def products(p):
        @pl.when(primary)
        def _():
            relay_step(p, R - 1)

        @pl.when(jnp.logical_not(primary))
        def _():
            for j in range(q):
                for u in range(C):
                    relay_copy(p, j, u).wait_recv()

        offsets = list(range(1, CX)) + [0]
        for near_side, o in [(True, o) for o in offsets] + [(False, o) for o in offsets]:
            ux = lax.rem(x + o, CX)
            u = ((1 - y) if near_side else y) * CX + ux

            @pl.loop(0, q * hb)
            def _(k):
                j, t = lax.div(k, hb), lax.rem(k, hb)
                keep = masks[p][u, c * q * hb + k] > 0
                rows = pl.ds(pl.multiple_of(t * B, B), B)
                blk = col[p, j, u, rows, :]
                rhs[pl.ds(pl.multiple_of(k * B, B), B), :] = jnp.where(
                    keep, blk, jnp.zeros_like(blk)
                )

            @pl.loop(0, hb)
            def _(t):
                rows = pl.ds(pl.multiple_of(t * B, B), B)
                v = jnp.dot(a_ref[rows, :], rhs[...], preferred_element_type=F32)
                if near_side:
                    part[p, ux, rows, :] = v.astype(BF)
                else:
                    acc[p, ux, rows, :] = v

            if near_side:
                near_copy(p, ux).start()

    def second(p):
        for o in range(1, CX):
            ux = lax.rem(x + o, CX)
            near_copy(p, ux).wait_recv()

            @pl.loop(0, hb)
            def _(t):
                rows = pl.ds(pl.multiple_of(t * B, B), B)
                sent[p, ux, rows, :] = (
                    acc[p, ux, rows, :] + near[p, ux, rows, :].astype(F32)
                ).astype(BF)

            last_copy(p, ux).start()

    def wait_parts(p):
        near_copy(p, x).wait_recv()
        for o in range(1, CX):
            ux = lax.rem(x + o, CX)
            copy(
                last.at[p, ux], last.at[p, ux], l_ss.at[p, ux], l_rs.at[p, ux], (g, z, y * CX + ux)
            ).wait_recv()

    def total(p, rows):
        v = acc[p, x, rows, :] + near[p, x, rows, :].astype(F32)
        for o in range(1, CX):
            v = v + last[p, lax.rem(x + o, CX), rows, :].astype(F32)
        return v

    def red_copy(k, o):
        i = lax.rem(r + o, n)
        return copy(
            part3.at[k, pl.ds(pl.multiple_of(i * S, S), S), :], red.at[k, r],
            red_ss.at[k, o], red_rs.at[k, r], rdev(i),
        )

    def send_sum(k):
        red[k, r] = part3[k, pl.ds(pl.multiple_of(r * S, S), S), :]
        for o in range(1, n):
            red_copy(k, o).start()

    def take_sum(k):
        for o in range(1, n):
            s = lax.rem(r + o, n)
            copy(
                red.at[k, s], red.at[k, s], red_ss.at[k, o], red_rs.at[k, s], rdev(s)
            ).wait_recv()
        v = red[k, 0]
        for i in range(1, n):
            v = v + red[k, i]
        return v

    mine = pl.ds(pl.multiple_of(r * S, S), S)

    def spread_copy(buf, ss, rs, o):
        return copy(buf.at[mine, :], buf.at[mine, :], ss.at[o], rs.at[r], rdev(lax.rem(r + o, n)))

    def spread(buf, ss, rs):
        for o in range(1, n):
            spread_copy(buf, ss, rs, o).start()

    def gathered(buf, ss, rs):
        for o in range(1, n):
            s = lax.rem(r + o, n)
            at = buf.at[pl.ds(pl.multiple_of(s * S, S), S), :]
            copy(at, at, ss.at[o], rs.at[s], rdev(s)).wait_recv()

    def x_copy(o):
        to = y * CX + lax.rem(x + o, CX)
        return copy(xall.at[c], xall.at[c], x_ss.at[o], x_rs.at[c], (g, z, to))

    def xy_copy(o):
        u = y * CX + lax.rem(x + o, CX)
        return copy(
            xall.at[u], xall.at[u], xy_ss.at[o], x_rs.at[u], (g, z, (1 - y) * CX + x)
        )

    def wait_x(u):
        copy(xall.at[u], xall.at[u], xy_ss.at[0], x_rs.at[u], (g, z, (1 - y) * CX + x)).wait_recv()

    def dp_copy(o):
        return copy(dpar.at[c], dpar.at[c], dp_ss.at[o], dp_rs.at[c], (g, z, lax.rem(c + o, C)))

    @pl.when(primary)
    def _():
        start_own(0)

    @pl.when(jnp.logical_not(primary))
    def _():
        pre_copy(0).start()
        pre_copy(1).start()

    @pl.loop(0, hb)
    def _(t):
        rows = pl.ds(pl.multiple_of(t * B, B), B)
        ub, lb = lu_ref[rows, :], ll_ref[rows, :]
        lum[rows, :] = jnp.where(mu_ref[c, r * hb + t] > 0, ub, jnp.zeros_like(ub))
        llm[rows, :] = jnp.where(ml_ref[c, r * hb + t] > 0, lb, jnp.zeros_like(lb))

    @pl.when(primary)
    def _():
        for s in range(1, R):
            row_step(0, s)
        start_own(1)
        row_step(1, 1)

    products(0)

    @pl.when(primary)
    def _():
        row_step(1, 2)

    second(0)

    @pl.when(primary)
    def _():
        for s in range(3, R):
            row_step(1, s)

    wait_parts(0)

    @pl.loop(0, hb)
    def _(t):
        rows = pl.ds(pl.multiple_of(t * B, B), B)
        v = (-total(0, rows)).astype(BF)
        xall[c, rows, :] = v
        x_ref[rows, :] = v

    for o in range(1, CX):
        x_copy(o).start()
    xy_copy(0).start()

    products(1)

    for o in range(1, CX):
        wait_x(y * CX + lax.rem(x + o, CX))
        xy_copy(o).start()
    part3[0] = tdot(lum[...], x_ref[...])
    send_sum(0)
    second(1)
    for o in range(CX):
        wait_x((1 - y) * CX + lax.rem(x + o, CX))
    here = par_ref[c]
    part3[1] = tdot(xall[here], llm[...])
    send_sum(1)

    dslice = (du_ref[mine, :] - take_sum(0)).astype(BF)
    dufull[mine, :] = dslice
    dpar[c] = dslice
    for o in range(1, C):
        dp_copy(o).start()
    spread(dufull, d_ss, d_rs)

    @pl.loop(0, hb)
    def _(t):
        rows = pl.ds(pl.multiple_of(t * B, B), B)
        acc[1, x, rows, :] += jnp.dot(xall[here, rows, :], lp_ref[...], preferred_element_type=F32)

    for o in range(1, C):
        s = lax.rem(c + o, C)
        copy(dpar.at[s], dpar.at[s], dp_ss.at[o], dp_rs.at[s], (g, z, s)).wait_recv()
    terms = jnp.dot(dpar[here], lp_ref[...], preferred_element_type=F32)
    ypfull[mine, :] = (-(take_sum(1) + terms)).astype(BF)
    spread(ypfull, y_ss, y_rs)

    wait_parts(1)

    @pl.loop(0, hb)
    def _(t):
        rows = pl.ds(pl.multiple_of(t * B, B), B)
        y_ref[rows, :] = (-total(1, rows)).astype(BF)

    part3[2] = tdot(llm[...], y_ref[...])
    send_sum(2)
    gathered(ypfull, y_ss, y_rs)
    back = tdot(lp_ref[...], ypfull[...])
    yp_ref[...] = ypfull[...]
    gathered(dufull, d_ss, d_rs)
    diagu_ref[...] = dufull[...]
    ownfull[mine, :] = take_sum(2)
    spread(ownfull, o_ss, o_rs)
    gathered(ownfull, o_ss, o_rs)
    diagl_ref[...] = (dl_ref[...] - ownfull[...] - back).astype(BF)

    for p in range(2):
        @pl.when(primary)
        def _():
            for z0 in range(R):
                for yy in range(G):
                    @pl.when(jnp.logical_and(z0 <= z, z < R - 1))
                    def _():
                        row_copy(p, z0, yy, 0).wait_send()

                    @pl.when(jnp.logical_and(z0 >= z, z > 0))
                    def _():
                        row_copy(p, z0, yy, 1).wait_send()

                    @pl.when(lax.div(g * R + z0, q) != c)
                    def _():
                        plane_copy(p, z0, yy, zbuf.at[p, z0, yy]).wait_send()

            for j in range(q):
                for u in range(C):
                    relay_copy(p, j, u).wait_send()

        @pl.when(jnp.logical_not(primary))
        def _():
            pre_copy(p).wait_send()

        for ux in range(CX):
            near_copy(p, ux).wait_send()
        for o in range(1, CX):
            last_copy(p, lax.rem(x + o, CX)).wait_send()
    for o in range(CX):
        xy_copy(o).wait_send()
    for o in range(1, CX):
        x_copy(o).wait_send()
    for o in range(1, C):
        dp_copy(o).wait_send()
    for o in range(1, n):
        for k in range(3):
            red_copy(k, o).wait_send()
        spread_copy(dufull, d_ss, d_rs, o).wait_send()
        spread_copy(ypfull, y_ss, y_rs, o).wait_send()
        spread_copy(ownfull, o_ss, o_rs, o).wait_send()


def on_device(G, R, C, a, lu, mu, du, ll, ml, par, lp, dl):
    h = lu.shape[0]
    n = G * R
    q = n // C
    S = B // n
    CX = C // G
    vm = pl.BlockSpec(memory_space=pltpu.VMEM)
    sm = pl.BlockSpec(memory_space=pltpu.SMEM)
    dma = pltpu.SemaphoreType.DMA
    small = jax.ShapeDtypeStruct((B, B), BF)
    tall = jax.ShapeDtypeStruct((h, B), BF)
    return pl.pallas_call(
        functools.partial(kernel, G, R, C),
        out_shape=(tall, small, tall, small, small),
        in_specs=[vm, vm, sm, vm, vm, sm, sm, vm, vm],
        out_specs=(vm,) * 5,
        scratch_shapes=[
            pltpu.VMEM((2, R, G, h, B), BF),
            pltpu.VMEM((2, q, C, h, B), BF),
            pltpu.VMEM((2, CX, h, B), BF),
            pltpu.VMEM((2, CX, h, B), BF),
            pltpu.VMEM((2, CX, h, B), BF),
            pltpu.VMEM((2, CX, h, B), BF),
            pltpu.VMEM((2, CX, h, B), F32),
            pltpu.VMEM((C, h, B), BF),
            pltpu.VMEM((q * h, B), BF),
            pltpu.VMEM((h, B), BF),
            pltpu.VMEM((h, B), BF),
            pltpu.VMEM((3, B, B), F32),
            pltpu.VMEM((3, n, S, B), F32),
            pltpu.VMEM((B, B), BF),
            pltpu.VMEM((C, S, B), BF),
            pltpu.VMEM((B, B), BF),
            pltpu.VMEM((B, B), F32),
            dma((2,)), dma((2, R, G, 2)), dma((2, R, G)), dma((2, R, G)), dma((2, q, C)),
            dma((2, q, C)), dma((2, CX)), dma((2, CX)), dma((2, CX)), dma((2, CX)),
            dma((CX,)), dma((C,)), dma((CX,)), dma((3, n)), dma((3, n)),
            dma((n,)), dma((n,)), dma((C,)), dma((C,)), dma((n,)), dma((n,)), dma((n,)), dma((n,)),
        ],
        compiler_params=pltpu.CompilerParams(
            collective_id=0, has_side_effects=True, vmem_limit_bytes=60 * 1024 * 1024
        ),
    )(a, lu, mu, du, ll, ml, par, lp, dl)


def solution(mesh):
    tall, wide = P(("grp", "row"), "col"), P(None, "col")
    return jax.shard_map(
        functools.partial(
            on_device, mesh.shape["grp"], mesh.shape["row"], mesh.shape["col"]
        ),
        mesh=mesh,
        in_specs=(tall, tall, P(), wide, tall, P(), P(), wide, wide),
        out_specs=(tall, wide, tall, wide, wide),
        check_vma=False,
    )
```

```python
import functools

import jax
import jax.numpy as jnp
from jax import lax
from jax.experimental import pallas as pl
from jax.experimental.pallas import tpu as pltpu
from jax.sharding import PartitionSpec as P

B = 256
MESH = pl.DeviceIdType.MESH
W = 2
BF = jnp.bfloat16
F32 = jnp.float32


def tdot(a, b):
    return lax.dot_general(a, b, (((0,), (0,)), ((), ())), preferred_element_type=F32)


def kernel(
    G, R, C,
    a_ref, lu_ref, mu_ref, du_ref, ll_ref, ml_ref, par_ref, lp_ref, dl_ref,
    x_ref, diagu_ref, y_ref, yp_ref, diagl_ref,
    zbuf, col, part, near, sent, last, acc, xall, rhs, lum, llm, part3, red, dufull, dpar,
    ypfull, ownfull,
    pre_ss, z_ss, z_rs, p_ss, c_rs, r_ss, n_ss, n_rs, l_ss, l_rs, x_ss, x_rs, xy_ss,
    red_ss, red_rs, d_ss, d_rs, dp_ss, dp_rs, y_ss, y_rs, o_ss, o_rs,
):
    g, z, c = lax.axis_index("grp"), lax.axis_index("row"), lax.axis_index("col")
    n = G * R
    q = n // C
    CX = C // G
    y, x = lax.div(c, CX), lax.rem(c, CX)
    r = g * R + z
    h = lu_ref.shape[0]
    hb = h // B
    S = B // n
    panels = (lu_ref, ll_ref)
    masks = (mu_ref, ml_ref)
    primary = y == g

    def rdev(i):
        return (lax.div(i, R), lax.rem(i, R), c)

    def copy(src, dst, ss, rs, dev):
        return pltpu.make_async_remote_copy(
            src_ref=src, dst_ref=dst, send_sem=ss, recv_sem=rs, device_id=dev, device_id_type=MESH
        )

    barrier = pltpu.get_barrier_semaphore()
    for o in range(1, n):
        pl.semaphore_signal(barrier, inc=1, device_id=rdev(lax.rem(r + o, n)), device_id_type=MESH)
    for o in range(1, C):
        pl.semaphore_signal(
            barrier, inc=1, device_id=(g, z, lax.rem(c + o, C)), device_id_type=MESH
        )
    pl.semaphore_wait(barrier, n - 1 + C - 1)

    def cutr(w):
        return pl.ds(w * (h // W), h // W)

    def pre_copy(p, w):
        return copy(
            panels[p].at[cutr(w), :], zbuf.at[p, z, y, cutr(w), :], pre_ss.at[p, w],
            z_rs.at[p, z, y, w], (g, z, g * CX + x),
        )

    def row_copy(p, z0, yy, side, w, own=False):
        to = z + 1 if side == 0 else z - 1
        at = zbuf.at[p, z0, yy, cutr(w), :]
        return copy(
            panels[p].at[cutr(w), :] if own else at, at, z_ss.at[p, z0, yy, side, w],
            z_rs.at[p, z0, yy, w], (g, to, c),
        )

    def piece(p, z0, yy, w, own):
        return panels[p].at[cutr(w), :] if own else zbuf.at[p, z0, yy, cutr(w), :]

    def plane_copy(p, z0, yy, w, own=False):
        r0 = g * R + z0
        u = yy * CX + x
        j = lax.rem(r0, q)
        return copy(
            piece(p, z0, yy, w, own), col.at[p, j, u, cutr(w), :], p_ss.at[p, z0, yy, w],
            c_rs.at[p, j, u, w], (g, z, lax.div(r0, q)),
        )

    def relay_copy(p, j, u, w):
        at = col.at[p, j, u, cutr(w), :]
        return copy(at, at, r_ss.at[p, j, u, w], c_rs.at[p, j, u, w], (1 - g, z, c))

    def to_plane(p, z0, yy, w, own):
        r0 = g * R + z0
        d = lax.div(r0, q)

        @pl.when(d == c)
        def _():
            j = lax.rem(r0, q)
            u = yy * CX + x
            pltpu.make_async_copy(
                piece(p, z0, yy, w, own), col.at[p, j, u, cutr(w), :], c_rs.at[p, j, u, w]
            ).start()

        @pl.when(d != c)
        def _():
            plane_copy(p, z0, yy, w, own).start()

    def pass_on(p, z0, yy, sides, w, own=False):
        if 0 in sides:
            @pl.when(z < R - 1)
            def _():
                row_copy(p, z0, yy, 0, w, own).start()

        if 1 in sides:
            @pl.when(z > 0)
            def _():
                row_copy(p, z0, yy, 1, w, own).start()

        to_plane(p, z0, yy, w, own)

    def start_own(p):
        for w in range(W):
            pass_on(p, z, g, (0, 1), w, True)
        for w in range(W):
            row_copy(p, z, 1 - g, 0, w).wait_recv()
            pass_on(p, z, 1 - g, (0, 1), w)

    def relay(p, z0):
        r0 = g * R + z0

        @pl.when(lax.div(r0, q) == c)
        def _():
            j = lax.rem(r0, q)
            for o in range(CX):
                for yy in range(G):
                    for w in range(W):
                        u = yy * CX + lax.rem(x + o, CX)
                        relay_copy(p, j, u, w).wait_recv()
                        relay_copy(p, j, u, w).start()

    def relay_step(p, s):
        if s < 0:
            return
        if s == 0:
            relay(p, z)
            return

        @pl.when(z - s >= 0)
        def _():
            relay(p, z - s)

        @pl.when(z + s < R)
        def _():
            relay(p, z + s)

    def row_step(p, s):
        zl, zr = z - s, z + s
        for i in range(G):
            for w in range(W):
                yy = lax.rem(g + i, G)

                @pl.when(zl >= 0)
                def _():
                    row_copy(p, zl, yy, 0, w).wait_recv()
                    pass_on(p, zl, yy, (0,), w)

                @pl.when(zr < R)
                def _():
                    row_copy(p, zr, yy, 1, w).wait_recv()
                    pass_on(p, zr, yy, (1,), w)

        relay_step(p, s - 2)

    def near_copy(p, ux):
        return copy(
            part.at[p, ux], near.at[p, ux], n_ss.at[p, ux], n_rs.at[p, ux], (g, z, (1 - y) * CX + x)
        )

    def last_copy(p, ux):
        return copy(
            sent.at[p, ux], last.at[p, x], l_ss.at[p, ux], l_rs.at[p, x], (g, z, y * CX + ux)
        )

    def products(p):
        @pl.when(primary)
        def _():
            for s in range(max(R - 2, 0), R):
                relay_step(p, s)

        @pl.when(jnp.logical_not(primary))
        def _():
            for j in range(q):
                for u in range(C):
                    for w in range(W):
                        relay_copy(p, j, u, w).wait_recv()

        offsets = list(range(1, CX)) + [0]
        for near_side, o in [(True, o) for o in offsets] + [(False, o) for o in offsets]:
            ux = lax.rem(x + o, CX)
            u = ((1 - y) if near_side else y) * CX + ux

            @pl.loop(0, q * hb)
            def _(k):
                j, t = lax.div(k, hb), lax.rem(k, hb)
                keep = masks[p][u, c * q * hb + k] > 0
                rows = pl.ds(pl.multiple_of(t * B, B), B)
                blk = col[p, j, u, rows, :]
                rhs[pl.ds(pl.multiple_of(k * B, B), B), :] = jnp.where(
                    keep, blk, jnp.zeros_like(blk)
                )

            @pl.loop(0, hb)
            def _(t):
                rows = pl.ds(pl.multiple_of(t * B, B), B)
                v = jnp.dot(a_ref[rows, :], rhs[...], preferred_element_type=F32)
                if near_side:
                    part[p, ux, rows, :] = v.astype(BF)
                else:
                    acc[p, ux, rows, :] = v

            if near_side:
                near_copy(p, ux).start()

    def second(p):
        for o in range(1, CX):
            ux = lax.rem(x + o, CX)
            near_copy(p, ux).wait_recv()

            @pl.loop(0, hb)
            def _(t):
                rows = pl.ds(pl.multiple_of(t * B, B), B)
                sent[p, ux, rows, :] = (
                    acc[p, ux, rows, :] + near[p, ux, rows, :].astype(F32)
                ).astype(BF)

            last_copy(p, ux).start()

    def wait_parts(p):
        near_copy(p, x).wait_recv()
        for o in range(1, CX):
            ux = lax.rem(x + o, CX)
            copy(
                last.at[p, ux], last.at[p, ux], l_ss.at[p, ux], l_rs.at[p, ux], (g, z, y * CX + ux)
            ).wait_recv()

    def total(p, rows):
        v = acc[p, x, rows, :] + near[p, x, rows, :].astype(F32)
        for o in range(1, CX):
            v = v + last[p, lax.rem(x + o, CX), rows, :].astype(F32)
        return v

    def red_copy(k, o):
        i = lax.rem(r + o, n)
        return copy(
            part3.at[k, pl.ds(pl.multiple_of(i * S, S), S), :], red.at[k, r],
            red_ss.at[k, o], red_rs.at[k, r], rdev(i),
        )

    def send_sum(k):
        red[k, r] = part3[k, pl.ds(pl.multiple_of(r * S, S), S), :]
        for o in range(1, n):
            red_copy(k, o).start()

    def take_sum(k):
        for o in range(1, n):
            s = lax.rem(r + o, n)
            copy(
                red.at[k, s], red.at[k, s], red_ss.at[k, o], red_rs.at[k, s], rdev(s)
            ).wait_recv()
        v = red[k, 0]
        for i in range(1, n):
            v = v + red[k, i]
        return v

    mine = pl.ds(pl.multiple_of(r * S, S), S)

    def spread_copy(buf, ss, rs, o):
        return copy(buf.at[mine, :], buf.at[mine, :], ss.at[o], rs.at[r], rdev(lax.rem(r + o, n)))

    def spread(buf, ss, rs):
        for o in range(1, n):
            spread_copy(buf, ss, rs, o).start()

    def gathered(buf, ss, rs):
        for o in range(1, n):
            s = lax.rem(r + o, n)
            at = buf.at[pl.ds(pl.multiple_of(s * S, S), S), :]
            copy(at, at, ss.at[o], rs.at[s], rdev(s)).wait_recv()

    def xn_copy():
        return copy(
            xall.at[c], xall.at[c], x_ss.at[0], x_rs.at[c], (g, z, (1 - y) * CX + x)
        )

    def xr_copy(o, yy):
        u = yy * CX + x
        return copy(
            xall.at[u], xall.at[u], xy_ss.at[o, yy], x_rs.at[u],
            (g, z, y * CX + lax.rem(x + o, CX)),
        )

    def wait_x(u):
        copy(xall.at[u], xall.at[u], x_ss.at[0], x_rs.at[u], (g, z, (1 - y) * CX + x)).wait_recv()

    def dp_copy(o):
        return copy(dpar.at[c], dpar.at[c], dp_ss.at[o], dp_rs.at[c], (g, z, lax.rem(c + o, C)))

    @pl.when(primary)
    def _():
        start_own(0)

    @pl.when(jnp.logical_not(primary))
    def _():
        for p in range(2):
            for w in range(W):
                pre_copy(p, w).start()

    @pl.loop(0, hb)
    def _(t):
        rows = pl.ds(pl.multiple_of(t * B, B), B)
        ub, lb = lu_ref[rows, :], ll_ref[rows, :]
        lum[rows, :] = jnp.where(mu_ref[c, r * hb + t] > 0, ub, jnp.zeros_like(ub))
        llm[rows, :] = jnp.where(ml_ref[c, r * hb + t] > 0, lb, jnp.zeros_like(lb))

    @pl.when(primary)
    def _():
        for s in range(1, R):
            row_step(0, s)
        start_own(1)
        row_step(1, 1)

    products(0)

    @pl.when(primary)
    def _():
        row_step(1, 2)

    second(0)

    @pl.when(primary)
    def _():
        for s in range(3, R):
            row_step(1, s)

    wait_parts(0)

    @pl.loop(0, hb)
    def _(t):
        rows = pl.ds(pl.multiple_of(t * B, B), B)
        v = (-total(0, rows)).astype(BF)
        xall[c, rows, :] = v
        x_ref[rows, :] = v

    xn_copy().start()
    for o in range(1, CX):
        xr_copy(o, y).start()

    products(1)

    wait_x((1 - y) * CX + x)
    for o in range(1, CX):
        xr_copy(o, 1 - y).start()
    part3[0] = tdot(lum[...], x_ref[...])
    send_sum(0)
    second(1)
    for o in range(1, CX):
        for yy in range(G):
            wait_x(yy * CX + lax.rem(x + o, CX))
    here = par_ref[c]
    part3[1] = tdot(xall[here], llm[...])
    send_sum(1)

    dslice = (du_ref[mine, :] - take_sum(0)).astype(BF)
    dufull[mine, :] = dslice
    dpar[c] = dslice
    for o in range(1, C):
        dp_copy(o).start()
    spread(dufull, d_ss, d_rs)

    @pl.loop(0, hb)
    def _(t):
        rows = pl.ds(pl.multiple_of(t * B, B), B)
        acc[1, x, rows, :] += jnp.dot(xall[here, rows, :], lp_ref[...], preferred_element_type=F32)

    for o in range(1, C):
        s = lax.rem(c + o, C)
        copy(dpar.at[s], dpar.at[s], dp_ss.at[o], dp_rs.at[s], (g, z, s)).wait_recv()
    terms = jnp.dot(dpar[here], lp_ref[...], preferred_element_type=F32)
    ypfull[mine, :] = (-(take_sum(1) + terms)).astype(BF)
    spread(ypfull, y_ss, y_rs)

    wait_parts(1)

    @pl.loop(0, hb)
    def _(t):
        rows = pl.ds(pl.multiple_of(t * B, B), B)
        y_ref[rows, :] = (-total(1, rows)).astype(BF)

    part3[2] = tdot(llm[...], y_ref[...])
    send_sum(2)
    gathered(ypfull, y_ss, y_rs)
    back = tdot(lp_ref[...], ypfull[...])
    yp_ref[...] = ypfull[...]
    gathered(dufull, d_ss, d_rs)
    diagu_ref[...] = dufull[...]
    ownfull[mine, :] = take_sum(2)
    spread(ownfull, o_ss, o_rs)
    gathered(ownfull, o_ss, o_rs)
    diagl_ref[...] = (dl_ref[...] - ownfull[...] - back).astype(BF)

    for p in range(2):
        @pl.when(primary)
        def _():
            for z0 in range(R):
                for yy in range(G):
                    for w in range(W):
                        @pl.when(jnp.logical_and(z0 <= z, z < R - 1))
                        def _():
                            row_copy(p, z0, yy, 0, w).wait_send()

                        @pl.when(jnp.logical_and(z0 >= z, z > 0))
                        def _():
                            row_copy(p, z0, yy, 1, w).wait_send()

                        @pl.when(lax.div(g * R + z0, q) != c)
                        def _():
                            plane_copy(p, z0, yy, w).wait_send()

            for j in range(q):
                for u in range(C):
                    for w in range(W):
                        relay_copy(p, j, u, w).wait_send()

        @pl.when(jnp.logical_not(primary))
        def _():
            for w in range(W):
                pre_copy(p, w).wait_send()

        for ux in range(CX):
            near_copy(p, ux).wait_send()
        for o in range(1, CX):
            last_copy(p, lax.rem(x + o, CX)).wait_send()
    xn_copy().wait_send()
    for o in range(1, CX):
        for yy in range(G):
            xr_copy(o, yy).wait_send()
    for o in range(1, C):
        dp_copy(o).wait_send()
    for o in range(1, n):
        for k in range(3):
            red_copy(k, o).wait_send()
        spread_copy(dufull, d_ss, d_rs, o).wait_send()
        spread_copy(ypfull, y_ss, y_rs, o).wait_send()
        spread_copy(ownfull, o_ss, o_rs, o).wait_send()


def on_device(G, R, C, a, lu, mu, du, ll, ml, par, lp, dl):
    h = lu.shape[0]
    n = G * R
    q = n // C
    S = B // n
    CX = C // G
    vm = pl.BlockSpec(memory_space=pltpu.VMEM)
    sm = pl.BlockSpec(memory_space=pltpu.SMEM)
    dma = pltpu.SemaphoreType.DMA
    small = jax.ShapeDtypeStruct((B, B), BF)
    tall = jax.ShapeDtypeStruct((h, B), BF)
    return pl.pallas_call(
        functools.partial(kernel, G, R, C),
        out_shape=(tall, small, tall, small, small),
        in_specs=[vm, vm, sm, vm, vm, sm, sm, vm, vm],
        out_specs=(vm,) * 5,
        scratch_shapes=[
            pltpu.VMEM((2, R, G, h, B), BF),
            pltpu.VMEM((2, q, C, h, B), BF),
            pltpu.VMEM((2, CX, h, B), BF),
            pltpu.VMEM((2, CX, h, B), BF),
            pltpu.VMEM((2, CX, h, B), BF),
            pltpu.VMEM((2, CX, h, B), BF),
            pltpu.VMEM((2, CX, h, B), F32),
            pltpu.VMEM((C, h, B), BF),
            pltpu.VMEM((q * h, B), BF),
            pltpu.VMEM((h, B), BF),
            pltpu.VMEM((h, B), BF),
            pltpu.VMEM((3, B, B), F32),
            pltpu.VMEM((3, n, S, B), F32),
            pltpu.VMEM((B, B), BF),
            pltpu.VMEM((C, S, B), BF),
            pltpu.VMEM((B, B), BF),
            pltpu.VMEM((B, B), F32),
            dma((2, W)), dma((2, R, G, 2, W)), dma((2, R, G, W)), dma((2, R, G, W)),
            dma((2, q, C, W)), dma((2, q, C, W)), dma((2, CX)), dma((2, CX)), dma((2, CX)), dma((2, CX)),
            dma((1,)), dma((C,)), dma((CX, G)), dma((3, n)), dma((3, n)),
            dma((n,)), dma((n,)), dma((C,)), dma((C,)), dma((n,)), dma((n,)), dma((n,)), dma((n,)),
        ],
        compiler_params=pltpu.CompilerParams(
            collective_id=0, has_side_effects=True, vmem_limit_bytes=60 * 1024 * 1024
        ),
    )(a, lu, mu, du, ll, ml, par, lp, dl)


def solution(mesh):
    tall, wide = P(("grp", "row"), "col"), P(None, "col")
    return jax.shard_map(
        functools.partial(
            on_device, mesh.shape["grp"], mesh.shape["row"], mesh.shape["col"]
        ),
        mesh=mesh,
        in_specs=(tall, tall, P(), wide, tall, P(), P(), wide, wide),
        out_specs=(tall, wide, tall, wide, wide),
        check_vma=False,
    )
```
